32 devices in a mesh: img: 8 (over y, x, core), atom: 4 (over z).
Axes of the slice: x: 2, y: 2, z: 4, core: 2. Of those that a mesh axis runs over, the one named last changes fastest.
Arguments:
- positions: float32 [3, 256, 4096], P(None, 'img', 'atom'), may hold values from -6 to 6
- strength: float32 [4096], replicated, may hold values from 0.5 to 2
- tile_pairs: int32 [32, 8], replicated, may hold values from 0 to 31
- source_segment: int32 [256], P('img'), may hold values from 1 to 255, as said below
Outputs:
- string: float32 [3, 256, 4096], P(None, 'img', 'atom')
The draws below stay inside these ranges and needn't reach their ends.
Inputs may be any that keep to these rules, and one draw needn't show every extreme that they name: source_segment[j] is j or j + 1, never 0 and never above 255.
All inputs are finite; a program needn't handle non-finite values.
Results may differ from the reference program's by a relative error of at most 0.0003.
Values sent between devices are 32-bit elements; how exact they have to be, the bound alone decides.
No kernel may reach another device: no remote copies, remote signals or barrier semaphores. Data moves between devices by JAX's collectives and lax.ppermute only.
A program may use at most 64 MiB of HBM per device.

```python
import math
import jax
import jax.numpy as jnp
from jax import lax

NA = 4096
TB = 128
K = 8
NBLK = 32
IMAGES = 256


def draw_source_segment(key, part):
    bump = jax.random.randint(key, (IMAGES,), 0, 2).astype(jnp.int32)
    return jnp.clip(jnp.arange(IMAGES, dtype=jnp.int32) + bump, 1, IMAGES - 1).astype(jnp.int32)


def touch_ends(result, own_key, low, largest):
    shape = result.shape
    spot = [jax.random.randint(jax.random.fold_in(own_key, axis), (), 0, shape[axis]) for axis in range(len(shape))]
    result = result.at[tuple(spot)].set(low)
    longest = shape.index(max(shape))
    spot[longest] = (spot[longest] + 1) % shape[longest]
    return result.at[tuple(spot)].set(largest)


def block_scale(key, dims, shards, low, high):
    def one(axis_at, parts):
        steps = jax.random.uniform(jax.random.fold_in(jax.random.fold_in(key, 6), axis_at), (parts,), jnp.float32, low / len(shards), high / len(shards))
        return jnp.repeat(jnp.exp(steps), dims[axis_at] // parts).reshape((-1,) + (1,) * (len(dims) - axis_at - 1))

    level = one(*shards[0])
    for cut in shards[1:]:
        level = level * one(*cut)
    return level


def bell_draw(key, dims, deviation, most, shards=(), kind=jnp.bfloat16):
    loudness = block_scale(key, dims, shards, -0.22, 0.18) if shards else 1.0
    array = jax.random.normal(key, dims, jnp.float32) * deviation * loudness
    return jnp.minimum(jnp.maximum(array, -most), most).astype(kind)


def setup_inputs(seed: int = 0) -> dict:
    arg_keys = jax.random.split(jax.random.key(seed), 5)
    positions = bell_draw(arg_keys[0], (3, IMAGES, NA), 1.0, 6.0, ((1, 8), (2, 4)), jnp.float32)
    strength = jnp.clip(jnp.exp(jax.random.uniform(arg_keys[1], (NA,), jnp.float32, math.log(0.5), math.log(2.0))), 0.5, 2.0)
    tile_pairs = touch_ends(jax.random.randint(arg_keys[2], (NBLK, K), 0, NBLK), jax.random.fold_in(arg_keys[2], 1), 0, NBLK - 1).astype(jnp.int32)
    source_segment = draw_source_segment(jax.random.fold_in(arg_keys[4], 71), 0)
    return dict(positions=positions, strength=strength, tile_pairs=tile_pairs, source_segment=source_segment)


STEP_SIZE = 0.02

def pair_force(block_pos, block_strength, whole_pos, strength, partners):
    force_sum = jnp.zeros(block_pos.shape, jnp.float32)
    for neighbor_slot in range(partners.shape[0]):
        first_atom = (partners[neighbor_slot] * TB).astype(jnp.int32)
        partner_pos = lax.dynamic_slice_in_dim(whole_pos, first_atom, TB, 2)
        partner_strength = lax.dynamic_slice_in_dim(strength, first_atom, TB, 0)
        differ = block_pos[:, :, :, None] - partner_pos[:, :, None, :]
        radius = lax.optimization_barrier(jnp.sum(differ * differ, axis=0))
        coupling = block_strength[None, :, None] * partner_strength[None, None, :] * jnp.exp(-0.5 * radius)
        force_sum = force_sum + lax.optimization_barrier(jnp.sum(differ * coupling[None], axis=3))
    return force_sum

def reference(positions, strength, tile_pairs, source_segment):
    blocks = positions.reshape(3, IMAGES, NBLK, TB).transpose(2, 0, 1, 3)

    def one_block(inputs):
        block_pos, index = inputs
        partners = tile_pairs[index]
        block_strength = lax.dynamic_slice_in_dim(strength, (index * TB).astype(jnp.int32), TB, 0)
        return pair_force(block_pos, block_strength, positions, strength, partners)
    forces = lax.map(one_block, (blocks, jnp.arange(NBLK, dtype=jnp.int32)))
    forces = forces.transpose(1, 2, 0, 3).reshape(3, IMAGES, NA)
    moved = positions + STEP_SIZE * forces
    deltas = moved[:, 1:] - moved[:, :-1]
    squares = lax.optimization_barrier(jnp.sum(deltas * deltas, axis=(0, 2)))
    lengths = jnp.concatenate([jnp.zeros((1,), jnp.float32), jnp.sqrt(1.0 + squares)])
    arc = jnp.cumsum(lengths)
    total_arc = arc[-1]
    target = jnp.arange(IMAGES).astype(jnp.float32) * (total_arc / (IMAGES - 1))
    lower = (source_segment - 1).astype(jnp.int32)
    weight = (target - arc[lower]) / lengths[source_segment]
    string = (1.0 - weight)[None, :, None] * moved[:, lower] + weight[None, :, None] * moved[:, source_segment]
    return string
```

```python
import jax
import jax.numpy as jnp
from jax import lax
from jax.experimental import pallas as pl
from jax.experimental.pallas import tpu as pltpu
from jax.sharding import PartitionSpec as P

TB = 128
ROWS = 8
FEATURE_BLOCKS = 7
DEPTH = 128
LOG2E = 1.4426950408889634
STEP_SIZE = 0.02


def three_parts(value):
    high = value.astype(jnp.bfloat16).astype(jnp.float32)
    rest = value - high
    middle = rest.astype(jnp.bfloat16).astype(jnp.float32)
    return high, middle, rest - middle


def force_kernel(pairs_ref, x_ref, strength_ref, out_ref, partner_ref, own_ref, sum_ref):
    images, _, atoms = x_ref.shape
    tiles = atoms // TB
    row = lax.broadcasted_iota(jnp.int32, (ROWS, atoms), 0)
    one = jnp.ones((ROWS, atoms), jnp.float32)
    zero = jnp.zeros((ROWS, atoms), jnp.float32)
    log_strength = jnp.log(strength_ref[...]) * LOG2E
    for pair in range(images // 2):
        partner_rows = []
        for side in range(2):
            x = x_ref[2 * pair + side]
            xh, xm, xl = three_parts(x)
            vh, vm, vl = three_parts(x * LOG2E)
            const = (-0.5 * LOG2E) * jnp.sum(x * x, axis=0, keepdims=True) + log_strength
            ch, cm, cl = three_parts(jnp.broadcast_to(const, (ROWS, atoms)))
            first = jnp.where(row == 0, ch, jnp.where(row == 1, cm, cl))
            c_partner = jnp.where(row < 3, first, jnp.where(row < 6, one, zero))
            second = jnp.where(row == 3, ch, jnp.where(row == 4, cm, cl))
            c_own = jnp.where(row < 3, one, jnp.where(row < 6, second, zero))
            partner_rows += [xh, xh, xm, xm, xh, xl, c_partner]
            own = [vh, vm, vh, vm, vl, vh, c_own]
            blank = [zero] * FEATURE_BLOCKS
            own = (own + blank if side == 0 else blank + own) + [zero] * (
                DEPTH // ROWS - 2 * FEATURE_BLOCKS
            )
            own = jnp.concatenate(own, axis=0).astype(jnp.bfloat16)
            tops = jnp.where(row == 3, one, xh)
            parts = jnp.concatenate([tops, xm, xl], axis=0).astype(jnp.bfloat16)
            for tile in range(tiles):
                cut = slice(tile * TB, (tile + 1) * TB)
                own_ref[pair, tile, :, side * TB : (side + 1) * TB] = own[:, cut]
                for half in range(2):
                    sum_ref[pair, tile, 24 * side : 24 * side + 24, half * TB : (half + 1) * TB] = (
                        parts[:, cut]
                    )
        partner_rows += [zero] * (DEPTH // ROWS - 2 * FEATURE_BLOCKS)
        partner = jnp.concatenate(partner_rows, axis=0)
        for tile in range(tiles):
            partner_ref[pair, tile] = partner[:, tile * TB : (tile + 1) * TB].T.astype(jnp.bfloat16)

    slots = pairs_ref.shape[1]

    def step(index, carry):
        pair = index // tiles
        tile = index % tiles
        own = own_ref[pair, tile]
        acc = jnp.zeros((48, 2 * TB), jnp.float32)
        for slot in range(slots):
            other = pairs_ref[tile, slot]
            power = jnp.dot(partner_ref[pair, other], own, preferred_element_type=jnp.float32)
            w = jnp.exp2(power)
            high = w.astype(jnp.bfloat16)
            low = (w - high.astype(jnp.float32)).astype(jnp.bfloat16)
            both = jnp.concatenate([high, low], axis=0)
            acc = acc + jnp.dot(sum_ref[pair, other], both, preferred_element_type=jnp.float32)
        lanes = pl.ds(pl.multiple_of(tile * TB, TB), TB)
        for side in range(2):
            part = acc[24 * side : 24 * side + 24, side * TB : (side + 1) * TB]
            total = part[0:8] + part[8:16] + part[16:24]
            x = x_ref[2 * pair + side, :, lanes]
            force = x * total[3:4] - total
            out_ref[2 * pair + side, :, lanes] = x + STEP_SIZE * force
        return carry

    lax.fori_loop(0, (images // 2) * tiles, step, 0)


def moved_images(x, strength, tile_pairs):
    images, _, atoms = x.shape
    tiles = atoms // TB
    pairs = images // 2
    vmem = pl.BlockSpec(memory_space=pltpu.VMEM)
    return pl.pallas_call(
        force_kernel,
        out_shape=jax.ShapeDtypeStruct(x.shape, jnp.float32),
        in_specs=[pl.BlockSpec(memory_space=pltpu.SMEM), vmem, vmem],
        out_specs=vmem,
        scratch_shapes=[
            pltpu.VMEM((pairs, tiles, TB, DEPTH), jnp.bfloat16),
            pltpu.VMEM((pairs, tiles, DEPTH, 2 * TB), jnp.bfloat16),
            pltpu.VMEM((pairs, tiles, 48, 2 * TB), jnp.bfloat16),
        ],
        name="force",
    )(tile_pairs, x, strength[None, :])


def shards(positions, strength, tile_pairs, source_segment):
    count = positions.shape[1]
    blocks = lax.axis_size("atom")
    mine = count // blocks
    images_total = count * lax.axis_size("img")
    own = lax.all_to_all(positions, "atom", split_axis=1, concat_axis=2, tiled=True)
    x = jnp.pad(own.transpose(1, 0, 2), ((0, 0), (0, ROWS - 3), (0, 0)))
    moved = moved_images(x, strength, tile_pairs)[:, :3]
    everyone = images_total // mine
    before = lax.ppermute(
        moved[mine - 1 :], ("img", "atom"), [(i, i + 1) for i in range(everyone - 1)]
    )
    segments = moved - jnp.concatenate([before, moved[: mine - 1]], axis=0)
    squares = jnp.sum(segments * segments, axis=(1, 2))
    first = lax.axis_index(("img", "atom")) * mine
    ids = first + jnp.arange(mine, dtype=jnp.int32)
    own_lengths = jnp.where(ids >= 1, jnp.sqrt(1.0 + squares), 0.0)
    lengths = lax.all_gather(own_lengths, ("img", "atom"), axis=0, tiled=True)
    back = lax.all_to_all(moved.transpose(1, 0, 2), "atom", split_axis=2, concat_axis=1, tiled=True)
    ends = lax.axis_size("img") - 1
    head = lax.ppermute(back[:, count - 1 :], "img", [(i, i + 1) for i in range(ends)])
    tail = lax.ppermute(back[:, :1], "img", [(i + 1, i) for i in range(ends)])
    numbers = lax.axis_index("img") * count + jnp.arange(count, dtype=jnp.int32)
    columns = jnp.arange(images_total, dtype=jnp.int32)[None, :]
    segment = source_segment[:, None]
    arc_low = jnp.sum(jnp.where(columns < segment, lengths[None, :], 0.0), axis=1)
    span = jnp.sum(jnp.where(columns == segment, lengths[None, :], 0.0), axis=1)
    target = numbers.astype(jnp.float32) * (jnp.sum(lengths) / (images_total - 1))
    weight = ((target - arc_low) / span)[None, :, None]
    later = (source_segment > numbers)[None, :, None]
    previous = jnp.concatenate([head, back[:, : count - 1]], axis=1)
    following = jnp.concatenate([back[:, 1:], tail], axis=1)
    low = jnp.where(later, back, previous)
    high = jnp.where(later, following, back)
    return (1.0 - weight) * low + weight * high


def solution(mesh):
    placed = (P(None, "img", "atom"), P(), P(), P("img"))
    return jax.shard_map(
        shards, mesh=mesh, in_specs=placed, out_specs=P(None, "img", "atom"), check_vma=False
    )
```

```python
import jax
import jax.numpy as jnp
from jax import lax
from jax.experimental import pallas as pl
from jax.experimental.pallas import tpu as pltpu
from jax.sharding import PartitionSpec as P

TB = 128
ROWS = 8
FEATURE_BLOCKS = 7
DEPTH = 128
LOG2E = 1.4426950408889634
STEP_SIZE = 0.02
UNROLL = 8


def three_parts(value):
    high = value.astype(jnp.bfloat16).astype(jnp.float32)
    rest = value - high
    middle = rest.astype(jnp.bfloat16).astype(jnp.float32)
    return high, middle, rest - middle


def force_kernel(
    pairs_ref, pos_ref, strength_ref, out_ref, x_ref, new_ref, partner_ref, own_ref, sum_ref
):
    images, _, atoms = x_ref.shape
    blocks, _, _, local_atoms = out_ref.shape
    tiles = atoms // TB
    row = lax.broadcasted_iota(jnp.int32, (ROWS, atoms), 0)
    one = jnp.ones((ROWS, atoms), jnp.float32)
    zero = jnp.zeros((ROWS, atoms), jnp.float32)
    log_strength = jnp.log(strength_ref[...]) * LOG2E
    for pair in range(images // 2):
        partner_rows = []
        for side in range(2):
            image = 2 * pair + side
            x_ref[image] = zero
            for part in range(3):
                x_ref[image, part : part + 1] = pos_ref[part, image : image + 1]
            x = x_ref[image]
            xh, xm, xl = three_parts(x)
            vh, vm, vl = three_parts(x * LOG2E)
            const = (-0.5 * LOG2E) * jnp.sum(x * x, axis=0, keepdims=True) + log_strength
            ch, cm, cl = three_parts(jnp.broadcast_to(const, (ROWS, atoms)))
            first = jnp.where(row == 0, ch, jnp.where(row == 1, cm, cl))
            c_partner = jnp.where(row < 3, first, jnp.where(row < 6, one, zero))
            second = jnp.where(row == 3, ch, jnp.where(row == 4, cm, cl))
            c_own = jnp.where(row < 3, one, jnp.where(row < 6, second, zero))
            partner_rows += [xh, xh, xm, xm, xh, xl, c_partner]
            own = [vh, vm, vh, vm, vl, vh, c_own]
            blank = [zero] * FEATURE_BLOCKS
            own = (own + blank if side == 0 else blank + own) + [zero] * (
                DEPTH // ROWS - 2 * FEATURE_BLOCKS
            )
            own = jnp.concatenate(own, axis=0).astype(jnp.bfloat16)
            tops = jnp.where(row == 3, one, xh)
            parts = jnp.concatenate([tops, xm, xl], axis=0).astype(jnp.bfloat16)
            for tile in range(tiles):
                cut = slice(tile * TB, (tile + 1) * TB)
                own_ref[pair, tile, :, side * TB : (side + 1) * TB] = own[:, cut]
                for half in range(2):
                    sum_ref[pair, tile, 24 * side : 24 * side + 24, half * TB : (half + 1) * TB] = (
                        parts[:, cut]
                    )
        partner_rows += [zero] * (DEPTH // ROWS - 2 * FEATURE_BLOCKS)
        partner = jnp.concatenate(partner_rows, axis=0)
        for tile in range(tiles):
            partner_ref[pair, tile] = partner[:, tile * TB : (tile + 1) * TB].T.astype(jnp.bfloat16)

    slots = pairs_ref.shape[1]

    def step(index, carry):
        pair = index // tiles
        tile = index % tiles
        own = own_ref[pair, tile]
        acc = jnp.zeros((48, 2 * TB), jnp.float32)
        for slot in range(slots):
            other = pairs_ref[tile, slot]
            power = jnp.dot(partner_ref[pair, other], own, preferred_element_type=jnp.float32)
            w = jnp.exp2(power)
            high = w.astype(jnp.bfloat16)
            low = (w - high.astype(jnp.float32)).astype(jnp.bfloat16)
            both = jnp.concatenate([high, low], axis=0)
            acc = acc + jnp.dot(sum_ref[pair, other], both, preferred_element_type=jnp.float32)
        lanes = pl.ds(pl.multiple_of(tile * TB, TB), TB)
        for side in range(2):
            part = acc[24 * side : 24 * side + 24, side * TB : (side + 1) * TB]
            total = part[0:8] + part[8:16] + part[16:24]
            x = x_ref[2 * pair + side, :, lanes]
            force = x * total[3:4] - total
            new_ref[2 * pair + side, :, lanes] = x + STEP_SIZE * force
        return carry

    lax.fori_loop(0, (images // 2) * tiles, step, 0, unroll=UNROLL)
    for image in range(images):
        for block in range(blocks):
            for part in range(3):
                out_ref[block, part, image : image + 1] = new_ref[
                    image, part : part + 1, block * local_atoms : (block + 1) * local_atoms
                ]


def moved_images(positions, strength, tile_pairs, blocks):
    _, images, atoms = positions.shape
    tiles = atoms // TB
    pairs = images // 2
    vmem = pl.BlockSpec(memory_space=pltpu.VMEM)
    return pl.pallas_call(
        force_kernel,
        out_shape=jax.ShapeDtypeStruct((blocks, 3, images, atoms // blocks), jnp.float32),
        in_specs=[pl.BlockSpec(memory_space=pltpu.SMEM), vmem, vmem],
        out_specs=vmem,
        scratch_shapes=[
            pltpu.VMEM((images, ROWS, atoms), jnp.float32),
            pltpu.VMEM((images, ROWS, atoms), jnp.float32),
            pltpu.VMEM((pairs, tiles, TB, DEPTH), jnp.bfloat16),
            pltpu.VMEM((pairs, tiles, DEPTH, 2 * TB), jnp.bfloat16),
            pltpu.VMEM((pairs, tiles, 48, 2 * TB), jnp.bfloat16),
        ],
        name="force",
    )(tile_pairs, positions, strength[None, :])


def shards(positions, strength, tile_pairs, source_segment):
    _, count, local_atoms = positions.shape
    blocks = lax.axis_size("atom")
    images_total = count * lax.axis_size("img")
    own = lax.all_to_all(positions, "atom", split_axis=1, concat_axis=2, tiled=True)
    moved = moved_images(own, strength, tile_pairs, blocks)
    back = lax.all_to_all(moved, "atom", split_axis=0, concat_axis=0, tiled=True)
    back = back.transpose(1, 0, 2, 3).reshape(3, count, local_atoms)
    ends = lax.axis_size("img") - 1
    head = lax.ppermute(back[:, count - 1 :], "img", [(i, i + 1) for i in range(ends)])
    tail = lax.ppermute(back[:, :1], "img", [(i + 1, i) for i in range(ends)])
    previous = jnp.concatenate([head, back[:, : count - 1]], axis=1)
    following = jnp.concatenate([back[:, 1:], tail], axis=1)
    numbers = lax.axis_index("img") * count + jnp.arange(count, dtype=jnp.int32)
    columns = jnp.arange(images_total, dtype=jnp.int32)[None, :]
    apart = back - previous
    partial_squares = jnp.sum(apart * apart, axis=(0, 2))
    spread = jnp.sum(jnp.where(columns == numbers[:, None], partial_squares[:, None], 0.0), axis=0)
    squares = lax.psum(spread, ("img", "atom"))
    lengths = jnp.where(columns[0] >= 1, jnp.sqrt(1.0 + squares), 0.0)
    segment = source_segment[:, None]
    arc_low = jnp.sum(jnp.where(columns < segment, lengths[None, :], 0.0), axis=1)
    span = jnp.sum(jnp.where(columns == segment, lengths[None, :], 0.0), axis=1)
    target = numbers.astype(jnp.float32) * (jnp.sum(lengths) / (images_total - 1))
    weight = ((target - arc_low) / span)[None, :, None]
    later = (source_segment > numbers)[None, :, None]
    low = jnp.where(later, back, previous)
    high = jnp.where(later, following, back)
    return (1.0 - weight) * low + weight * high


def solution(mesh):
    placed = (P(None, "img", "atom"), P(), P(), P("img"))
    return jax.shard_map(
        shards, mesh=mesh, in_specs=placed, out_specs=P(None, "img", "atom"), check_vma=False
    )
```

```python
import jax
import jax.numpy as jnp
from jax import lax
from jax.experimental import pallas as pl
from jax.experimental.pallas import tpu as pltpu
from jax.sharding import PartitionSpec as P

TB = 128
ROWS = 8
FEATURE_BLOCKS = 7
DEPTH = 128
LOG2E = 1.4426950408889634
STEP_SIZE = 0.02
UNROLL = 8


def three_parts(value):
    high = value.astype(jnp.bfloat16).astype(jnp.float32)
    rest = value - high
    middle = rest.astype(jnp.bfloat16).astype(jnp.float32)
    return high, middle, rest - middle


def force_kernel(
    place_ref, pairs_ref, pos_ref, strength_ref, out_ref, x_ref, new_ref, partner_ref, own_ref, sum_ref
):
    images, _, atoms = x_ref.shape
    blocks, _, _, local_atoms = out_ref.shape
    place = place_ref[0]
    tiles = atoms // TB
    row = lax.broadcasted_iota(jnp.int32, (ROWS, atoms), 0)
    one = jnp.ones((ROWS, atoms), jnp.float32)
    zero = jnp.zeros((ROWS, atoms), jnp.float32)
    log_strength = jnp.log(strength_ref[...]) * LOG2E
    for pair in range(images // 2):
        partner_rows = []
        for side in range(2):
            image = 2 * pair + side
            x_ref[image] = zero
            for block in range(blocks):
                turn = lax.rem(place - block + blocks, blocks)
                cut = slice(block * local_atoms, (block + 1) * local_atoms)
                for part in range(3):
                    x_ref[image, part : part + 1, cut] = pos_ref[turn, part, image : image + 1]
            x = x_ref[image]
            xh, xm, xl = three_parts(x)
            vh, vm, vl = three_parts(x * LOG2E)
            const = (-0.5 * LOG2E) * jnp.sum(x * x, axis=0, keepdims=True) + log_strength
            ch, cm, cl = three_parts(jnp.broadcast_to(const, (ROWS, atoms)))
            first = jnp.where(row == 0, ch, jnp.where(row == 1, cm, cl))
            c_partner = jnp.where(row < 3, first, jnp.where(row < 6, one, zero))
            second = jnp.where(row == 3, ch, jnp.where(row == 4, cm, cl))
            c_own = jnp.where(row < 3, one, jnp.where(row < 6, second, zero))
            partner_rows += [xh, xh, xm, xm, xh, xl, c_partner]
            own = [vh, vm, vh, vm, vl, vh, c_own]
            blank = [zero] * FEATURE_BLOCKS
            own = (own + blank if side == 0 else blank + own) + [zero] * (
                DEPTH // ROWS - 2 * FEATURE_BLOCKS
            )
            own = jnp.concatenate(own, axis=0).astype(jnp.bfloat16)
            tops = jnp.where(row == 3, one, xh)
            parts = jnp.concatenate([tops, xm, xl], axis=0).astype(jnp.bfloat16)
            for tile in range(tiles):
                cut = slice(tile * TB, (tile + 1) * TB)
                own_ref[pair, tile, :, side * TB : (side + 1) * TB] = own[:, cut]
                for half in range(2):
                    sum_ref[pair, tile, 24 * side : 24 * side + 24, half * TB : (half + 1) * TB] = (
                        parts[:, cut]
                    )
        partner_rows += [zero] * (DEPTH // ROWS - 2 * FEATURE_BLOCKS)
        partner = jnp.concatenate(partner_rows, axis=0)
        for tile in range(tiles):
            partner_ref[pair, tile] = partner[:, tile * TB : (tile + 1) * TB].T.astype(jnp.bfloat16)

    slots = pairs_ref.shape[1]

    def step(index, carry):
        pair = index // tiles
        tile = index % tiles
        own = own_ref[pair, tile]
        acc = jnp.zeros((48, 2 * TB), jnp.float32)
        for slot in range(slots):
            other = pairs_ref[tile, slot]
            power = jnp.dot(partner_ref[pair, other], own, preferred_element_type=jnp.float32)
            w = jnp.exp2(power)
            high = w.astype(jnp.bfloat16)
            low = (w - high.astype(jnp.float32)).astype(jnp.bfloat16)
            both = jnp.concatenate([high, low], axis=0)
            acc = acc + jnp.dot(sum_ref[pair, other], both, preferred_element_type=jnp.float32)
        lanes = pl.ds(pl.multiple_of(tile * TB, TB), TB)
        for side in range(2):
            part = acc[24 * side : 24 * side + 24, side * TB : (side + 1) * TB]
            total = part[0:8] + part[8:16] + part[16:24]
            x = x_ref[2 * pair + side, :, lanes]
            force = x * total[3:4] - total
            new_ref[2 * pair + side, :, lanes] = x + STEP_SIZE * force
        return carry

    lax.fori_loop(0, (images // 2) * tiles, step, 0, unroll=UNROLL)
    for block in range(blocks):
        turn = lax.rem(block - place + blocks, blocks)
        for image in range(images):
            for part in range(3):
                out_ref[turn, part, image : image + 1] = new_ref[
                    image, part : part + 1, block * local_atoms : (block + 1) * local_atoms
                ]


def moved_images(place, pieces, strength, tile_pairs):
    blocks, _, images, local_atoms = pieces.shape
    atoms = blocks * local_atoms
    tiles = atoms // TB
    pairs = images // 2
    vmem = pl.BlockSpec(memory_space=pltpu.VMEM)
    smem = pl.BlockSpec(memory_space=pltpu.SMEM)
    return pl.pallas_call(
        force_kernel,
        out_shape=jax.ShapeDtypeStruct(pieces.shape, jnp.float32),
        in_specs=[smem, smem, vmem, vmem],
        out_specs=vmem,
        scratch_shapes=[
            pltpu.VMEM((images, ROWS, atoms), jnp.float32),
            pltpu.VMEM((images, ROWS, atoms), jnp.float32),
            pltpu.VMEM((pairs, tiles, TB, DEPTH), jnp.bfloat16),
            pltpu.VMEM((pairs, tiles, DEPTH, 2 * TB), jnp.bfloat16),
            pltpu.VMEM((pairs, tiles, 48, 2 * TB), jnp.bfloat16),
        ],
        name="force",
    )(place[None], tile_pairs, pieces, strength[None, :])


def exchanged(pieces):
    blocks = len(pieces)
    received = [pieces[0]] + [
        lax.ppermute(pieces[turn], "atom", [(i, (i + turn) % blocks) for i in range(blocks)])
        for turn in range(1, blocks)
    ]
    return jnp.stack(received)


def shards(positions, strength, tile_pairs, source_segment):
    count = positions.shape[1]
    blocks = lax.axis_size("atom")
    images_total = count * lax.axis_size("img")
    mine = count // blocks
    place = lax.axis_index("atom").astype(jnp.int32)
    outgoing = [
        lax.dynamic_slice_in_dim(positions, lax.rem(place + turn, blocks) * mine, mine, 1)
        for turn in range(blocks)
    ]
    moved = moved_images(place, exchanged(outgoing), strength, tile_pairs)
    returned = exchanged([moved[turn] for turn in range(blocks)])
    back = jnp.concatenate(
        [
            lax.dynamic_index_in_dim(
                returned, lax.rem(place - block + blocks, blocks), 0, keepdims=False
            )
            for block in range(blocks)
        ],
        axis=1,
    )
    ends = lax.axis_size("img") - 1
    head = lax.ppermute(back[:, count - 1 :], "img", [(i, i + 1) for i in range(ends)])
    tail = lax.ppermute(back[:, :1], "img", [(i + 1, i) for i in range(ends)])
    previous = jnp.concatenate([head, back[:, : count - 1]], axis=1)
    following = jnp.concatenate([back[:, 1:], tail], axis=1)
    numbers = lax.axis_index("img") * count + jnp.arange(count, dtype=jnp.int32)
    columns = jnp.arange(images_total, dtype=jnp.int32)[None, :]
    apart = back - previous
    partial_squares = jnp.sum(apart * apart, axis=(0, 2))
    squares = lax.psum(partial_squares, "atom")
    own_lengths = jnp.where(numbers >= 1, jnp.sqrt(1.0 + squares), 0.0)
    lengths = lax.all_gather(own_lengths, "img", axis=0, tiled=True)
    segment = source_segment[:, None]
    arc_low = jnp.sum(jnp.where(columns < segment, lengths[None, :], 0.0), axis=1)
    span = jnp.sum(jnp.where(columns == segment, lengths[None, :], 0.0), axis=1)
    target = numbers.astype(jnp.float32) * (jnp.sum(lengths) / (images_total - 1))
    weight = ((target - arc_low) / span)[None, :, None]
    later = (source_segment > numbers)[None, :, None]
    low = jnp.where(later, back, previous)
    high = jnp.where(later, following, back)
    return (1.0 - weight) * low + weight * high


def solution(mesh):
    placed = (P(None, "img", "atom"), P(), P(), P("img"))
    return jax.shard_map(
        shards, mesh=mesh, in_specs=placed, out_specs=P(None, "img", "atom"), check_vma=False
    )
```

```python
import jax
import jax.numpy as jnp
from jax import lax
from jax.experimental import pallas as pl
from jax.experimental.pallas import tpu as pltpu
from jax.sharding import PartitionSpec as P

TB = 128
ROWS = 8
FEATURE_BLOCKS = 7
DEPTH = 128
LOG2E = 1.4426950408889634
STEP_SIZE = 0.02
UNROLL = 16


def three_parts(value):
    high = value.astype(jnp.bfloat16).astype(jnp.float32)
    rest = value - high
    middle = rest.astype(jnp.bfloat16).astype(jnp.float32)
    return high, middle, rest - middle


def force_kernel(
    place_ref, pairs_ref, pos_ref, strength_ref, out_ref, x_ref, new_ref, partner_ref, own_ref, sum_ref
):
    images, _, atoms = x_ref.shape
    blocks, _, _, local_atoms = out_ref.shape
    place = place_ref[0]
    tiles = atoms // TB
    row = lax.broadcasted_iota(jnp.int32, (ROWS, atoms), 0)
    one = jnp.ones((ROWS, atoms), jnp.float32)
    zero = jnp.zeros((ROWS, atoms), jnp.float32)
    log_strength = jnp.log(strength_ref[...]) * LOG2E
    for pair in range(images // 2):
        partner_rows = []
        for side in range(2):
            image = 2 * pair + side
            x_ref[image] = zero
            for block in range(blocks):
                turn = lax.rem(place - block + blocks, blocks)
                cut = slice(block * local_atoms, (block + 1) * local_atoms)
                for part in range(3):
                    x_ref[image, part : part + 1, cut] = pos_ref[turn, part, image : image + 1]
            x = x_ref[image]
            xh, xm, xl = three_parts(x)
            vh, vm, vl = three_parts(x * LOG2E)
            const = (-0.5 * LOG2E) * jnp.sum(x * x, axis=0, keepdims=True) + log_strength
            ch, cm, cl = three_parts(jnp.broadcast_to(const, (ROWS, atoms)))
            first = jnp.where(row == 0, ch, jnp.where(row == 1, cm, cl))
            c_partner = jnp.where(row < 3, first, jnp.where(row < 6, one, zero))
            second = jnp.where(row == 3, ch, jnp.where(row == 4, cm, cl))
            c_own = jnp.where(row < 3, one, jnp.where(row < 6, second, zero))
            partner_rows += [xh, xh, xm, xm, xh, xl, c_partner]
            own = [vh, vm, vh, vm, vl, vh, c_own]
            blank = [zero] * FEATURE_BLOCKS
            own = (own + blank if side == 0 else blank + own) + [zero] * (
                DEPTH // ROWS - 2 * FEATURE_BLOCKS
            )
            own = jnp.concatenate(own, axis=0).astype(jnp.bfloat16)
            tops = jnp.where(row == 3, one, xh)
            parts = jnp.concatenate([tops, xm, xl], axis=0).astype(jnp.bfloat16)
            for tile in range(tiles):
                cut = slice(tile * TB, (tile + 1) * TB)
                own_ref[pair, tile, :, side * TB : (side + 1) * TB] = own[:, cut]
                for half in range(2):
                    sum_ref[pair, tile, 24 * side : 24 * side + 24, half * TB : (half + 1) * TB] = (
                        parts[:, cut]
                    )
        partner_rows += [zero] * (DEPTH // ROWS - 2 * FEATURE_BLOCKS)
        partner = jnp.concatenate(partner_rows, axis=0)
        for tile in range(tiles):
            partner_ref[pair, tile] = partner[:, tile * TB : (tile + 1) * TB].T.astype(jnp.bfloat16)

    slots = pairs_ref.shape[1]

    def step(index, carry):
        pair = index // tiles
        tile = index % tiles
        own = own_ref[pair, tile]
        acc = jnp.zeros((48, 2 * TB), jnp.float32)
        for slot in range(slots):
            other = pairs_ref[tile, slot]
            power = jnp.dot(partner_ref[pair, other], own, preferred_element_type=jnp.float32)
            w = jnp.exp2(power)
            high = w.astype(jnp.bfloat16)
            low = (w - high.astype(jnp.float32)).astype(jnp.bfloat16)
            both = jnp.concatenate([high, low], axis=0)
            acc = acc + jnp.dot(sum_ref[pair, other], both, preferred_element_type=jnp.float32)
        lanes = pl.ds(pl.multiple_of(tile * TB, TB), TB)
        for side in range(2):
            part = acc[24 * side : 24 * side + 24, side * TB : (side + 1) * TB]
            total = part[0:8] + part[8:16] + part[16:24]
            x = x_ref[2 * pair + side, :, lanes]
            force = x * total[3:4] - total
            new_ref[2 * pair + side, :, lanes] = x + STEP_SIZE * force
        return carry

    lax.fori_loop(0, (images // 2) * tiles, step, 0, unroll=UNROLL)
    for block in range(blocks):
        turn = lax.rem(block - place + blocks, blocks)
        for image in range(images):
            for part in range(3):
                out_ref[turn, part, image : image + 1] = new_ref[
                    image, part : part + 1, block * local_atoms : (block + 1) * local_atoms
                ]


def moved_images(place, pieces, strength, tile_pairs):
    blocks, _, images, local_atoms = pieces.shape
    atoms = blocks * local_atoms
    tiles = atoms // TB
    pairs = images // 2
    vmem = pl.BlockSpec(memory_space=pltpu.VMEM)
    smem = pl.BlockSpec(memory_space=pltpu.SMEM)
    return pl.pallas_call(
        force_kernel,
        out_shape=jax.ShapeDtypeStruct(pieces.shape, jnp.float32),
        in_specs=[smem, smem, vmem, vmem],
        out_specs=vmem,
        scratch_shapes=[
            pltpu.VMEM((images, ROWS, atoms), jnp.float32),
            pltpu.VMEM((images, ROWS, atoms), jnp.float32),
            pltpu.VMEM((pairs, tiles, TB, DEPTH), jnp.bfloat16),
            pltpu.VMEM((pairs, tiles, DEPTH, 2 * TB), jnp.bfloat16),
            pltpu.VMEM((pairs, tiles, 48, 2 * TB), jnp.bfloat16),
        ],
        name="force",
    )(place[None], tile_pairs, pieces, strength[None, :])


def exchanged(pieces):
    blocks = len(pieces)
    received = [pieces[0]] + [
        lax.ppermute(pieces[turn], "atom", [(i, (i + turn) % blocks) for i in range(blocks)])
        for turn in range(1, blocks)
    ]
    return jnp.stack(received)


def shards(positions, strength, tile_pairs, source_segment):
    count = positions.shape[1]
    blocks = lax.axis_size("atom")
    images_total = count * lax.axis_size("img")
    mine = count // blocks
    place = lax.axis_index("atom").astype(jnp.int32)
    outgoing = [
        lax.dynamic_slice_in_dim(positions, lax.rem(place + turn, blocks) * mine, mine, 1)
        for turn in range(blocks)
    ]
    moved = moved_images(place, exchanged(outgoing), strength, tile_pairs)
    returned = exchanged([moved[turn] for turn in range(blocks)])
    back = jnp.concatenate(
        [
            lax.dynamic_index_in_dim(
                returned, lax.rem(place - block + blocks, blocks), 0, keepdims=False
            )
            for block in range(blocks)
        ],
        axis=1,
    )
    ends = lax.axis_size("img") - 1
    head = lax.ppermute(back[:, count - 1 :], "img", [(i, i + 1) for i in range(ends)])
    tail = lax.ppermute(back[:, :1], "img", [(i + 1, i) for i in range(ends)])
    previous = jnp.concatenate([head, back[:, : count - 1]], axis=1)
    following = jnp.concatenate([back[:, 1:], tail], axis=1)
    numbers = lax.axis_index("img") * count + jnp.arange(count, dtype=jnp.int32)
    columns = jnp.arange(images_total, dtype=jnp.int32)[None, :]
    apart = back - previous
    partial_squares = jnp.sum(apart * apart, axis=(0, 2))
    squares = jnp.sum(exchanged([partial_squares] * blocks), axis=0)
    own_lengths = jnp.where(numbers >= 1, jnp.sqrt(1.0 + squares), 0.0)
    lengths = lax.all_gather(own_lengths, "img", axis=0, tiled=True)
    segment = source_segment[:, None]
    arc_low = jnp.sum(jnp.where(columns < segment, lengths[None, :], 0.0), axis=1)
    span = jnp.sum(jnp.where(columns == segment, lengths[None, :], 0.0), axis=1)
    target = numbers.astype(jnp.float32) * (jnp.sum(lengths) / (images_total - 1))
    weight = ((target - arc_low) / span)[None, :, None]
    later = (source_segment > numbers)[None, :, None]
    low = jnp.where(later, back, previous)
    high = jnp.where(later, following, back)
    return (1.0 - weight) * low + weight * high


def solution(mesh):
    placed = (P(None, "img", "atom"), P(), P(), P("img"))
    return jax.shard_map(
        shards, mesh=mesh, in_specs=placed, out_specs=P(None, "img", "atom"), check_vma=False
    )
```
